32 devices in a mesh: rep: 2 (over y), ep: 8 (over z, x), tp: 2 (over core).
Axes of the slice: x: 2, y: 2, z: 4, core: 2. Of those that a mesh axis runs over, the one named last changes fastest.
Arguments:
- residual_in: bfloat16 [2048, 4096], P(('rep', 'ep'), 'tp'), parts along dimension 0, may hold values from -3.2 to 3.2
- queries: bfloat16 [2048, 4096], P(('rep', 'ep'), 'tp'), parts along dimension 0, may hold values from -120 to 120
- key_rows: bfloat16 [2048, 256], P(('rep', 'ep')), parts along dimension 0, may hold values from -4 to 4
- value_rows: bfloat16 [2048, 256], P(('rep', 'ep')), parts along dimension 0, may hold values from -6 to 6
- seq_lengths: int32 [16], P(('rep', 'ep')), parts along dimension 0, may hold values from 64 to 128
- out_weight: bfloat16 [4096, 4096], P('tp', 'ep'), may hold values from -0.09375 to 0.09375
- norm_gain: float32 [4096], P('tp'), may hold values from 0.25 to 1.75
- expert_ids: int32 [2048, 8], P(('rep', 'ep')), parts along dimension 0, may hold values from 0 to 15, all different within a row; in each aligned block of 128 rows (0 to 127, 128 to 255, ...) at most 96 rows name the same one
- gate_probs: float32 [2048, 8], P(('rep', 'ep')), parts along dimension 0, may hold values from 0.03 to 0.5
- gate_weight: bfloat16 [16, 4096, 1536], P('ep', None, 'tp'), may hold values from -0.09375 to 0.09375
- up_weight: bfloat16 [16, 4096, 1536], P('ep', None, 'tp'), may hold values from -0.09375 to 0.09375
- down_weight: bfloat16 [16, 1536, 4096], P('ep', None, 'tp'), may hold values from -0.15625 to 0.15625
Outputs:
- layer_out: bfloat16 [2048, 4096], P(('rep', 'ep'), 'tp'), parts along dimension 0
The draws below stay inside these ranges and needn't reach their ends.
There are 2 independent parts, one for each index of `rep`. The reference program is written for one: setup_inputs(seed, part) draws one part's arguments, and reference() takes and returns one part's arrays. A program takes and returns all parts, laid end to end along the dimension named above; an argument that names none is the same for every part. Nothing has to cross between parts.
Inputs may be any that keep to these rules, and one draw needn't show every extreme that they name: `expert_ids`: each row names 8 different experts. Within the rows of one sequence no expert is named by more than 96 rows, a bound that some block reaches. `seq_lengths`: each sequence's number of valid tokens.
All inputs are finite; a program needn't handle non-finite values.
Results may differ from the reference program's by a relative error of at most 0.015.
Values may be sent and summed in bfloat16 or wider, within the bound.
A program may use at most 128 MiB of HBM per device.

```python
import math
import jax
import jax.numpy as jnp
import numpy as np
from jax import lax

D = 4096
HEADS = 32
KV_HEADS = 2
HEAD_DIM = 128
FF = 1536
TOP = 8
SEQ = 128
EXPERTS = 16
TOKENS = 1024
CAP = 96
N_EP = 8


def base_keys(key):
    raw = jax.random.normal(jax.random.fold_in(key, 71), (TOKENS, KV_HEADS * HEAD_DIM), jnp.float32)
    return jnp.clip(raw, -4.0, 4.0)


def draw_key_rows(key, part):
    keys_wide = base_keys(key)
    return keys_wide.astype(jnp.bfloat16)


def draw_queries(key, part):
    raw = jax.random.normal(jax.random.fold_in(key, 72), (TOKENS, HEADS * HEAD_DIM), jnp.float32)
    result = jnp.clip(raw, -4.0, 4.0)
    return result.astype(jnp.bfloat16)


def draw_residual_in(key, part):
    column_scale = 0.4 + 0.8 * jnp.arange(D, dtype=jnp.float32) / D
    values = jnp.clip(jax.random.normal(jax.random.fold_in(key, 81), (TOKENS, D), jnp.float32), -4.0, 4.0)
    return (0.5 * values * column_scale[None, :]).astype(jnp.bfloat16)


def with_ends(values, rng, smallest, high):
    shape = values.shape
    spot = [jax.random.randint(jax.random.fold_in(rng, axis), (), 0, shape[axis]) for axis in range(len(shape))]
    values = values.at[tuple(spot)].set(smallest)
    longest = shape.index(max(shape))
    spot[longest] = (spot[longest] + 1) % shape[longest]
    return values.at[tuple(spot)].set(high)


def shard_levels(key, shape, shards, smallest, top_value):
    loudness = 1.0
    for dim, shards_of in shards:
        steps = jax.random.uniform(jax.random.fold_in(jax.random.fold_in(key, 6), dim), (shards_of,), jnp.float32, smallest / len(shards), top_value / len(shards))
        loudness = loudness * jnp.repeat(jnp.exp(steps), shape[dim] // shards_of).reshape((-1,) + (1,) * (len(shape) - 1 - dim))
    return loudness


def routed_block(stream_key, own, number, rows, number_of, top, most, skew):
    ranking = jax.random.permutation(stream_key, number_of)
    crowded, common = portions_of(number_of, rows * top, most, skew, True), portions_of(number_of, rows * top, most, skew, False)
    places = jnp.arange(number_of)

    def named(sizes, offset_by):
        used = int((sizes > 0).sum())
        fixed = max(1, used // 4)
        passed = fixed + (places - fixed + offset_by * (used - fixed)) % max(1, number_of - fixed)
        return jnp.zeros((number_of,), jnp.int32).at[ranking[jnp.where(places < fixed, places, passed)]].set(jnp.asarray(sizes, jnp.int32))

    sizes = jnp.where(number % 4 == 0, named(crowded, number // 4), named(common, number - number // 4 - 1))
    mixed = jax.random.permutation(jax.random.fold_in(own, 3), number_of)
    giver, sink = mixed[0:number_of // 2 * 2:2], mixed[1:number_of // 2 * 2:2]
    slack = jnp.minimum(sizes[giver] - 1, most - sizes[sink]) // 2
    slack = jnp.where((giver == ranking[0]) | (sink == ranking[0]) | (sizes[sink] == 0), 0, jnp.maximum(slack, 0))
    passed = jax.random.randint(jax.random.fold_in(own, 4), (number_of // 2,), 0, 1 << 20) % (slack + 1)
    sizes = sizes.at[giver].add(-passed).at[sink].add(passed)
    members = jnp.searchsorted(jnp.cumsum(sizes), jnp.arange(rows * top), side="right").astype(jnp.int32)
    table = members.reshape(top, rows).T
    table = table[jax.random.permutation(jax.random.fold_in(own, 1), rows)]
    offset_by = jax.random.randint(jax.random.fold_in(own, 2), (rows, 1), 0, top)
    return jnp.take_along_axis(table, (jnp.arange(top)[None, :] + offset_by) % top, axis=1)


def portions_of(amount, total, bound, lean, full):
    loads = [(1 << 20) // math.isqrt(grade ** lean) + 1 for grade in range(1, amount + 1)]
    largest = bound if full else min(bound, max(-(-total // amount), total * loads[0] // sum(loads)))
    least = 1 if total - largest >= amount - 1 else 0
    given, rest = [largest] + [least] * (amount - 1), total - largest - least * (amount - 1)
    while rest > 0:
        free = [i for i in range(1, amount) if given[i] < largest] or [i for i in range(1, amount) if given[i] < bound]
        whole, left = sum([loads[i] for i in free]), rest
        for i in free:
            addition = min(bound - given[i], max(1, left * loads[i] // whole), rest)
            given[i] = given[i] + addition
            rest = rest - addition
    return np.array(given)


def gaussian(own_key, dims, spread, most, pieces=(), kind=jnp.bfloat16):
    drawn = spread * jax.random.normal(own_key, dims, jnp.float32)
    if pieces:
        drawn = drawn * shard_levels(own_key, dims, pieces, -0.22, 0.18)
    return jnp.clip(drawn, -most, most).astype(kind)


def setup_inputs(seed: int = 0, part: int = 0) -> dict:
    keys = jax.random.split(jax.random.key(seed), 13)
    part_keys = jax.random.split(jax.random.fold_in(keys[12], part), 13)
    residual_in = draw_residual_in(jax.random.fold_in(jax.random.fold_in(keys[12], part), 71), part)
    queries = draw_queries(jax.random.fold_in(jax.random.fold_in(keys[12], part), 71), part)
    key_rows = draw_key_rows(jax.random.fold_in(jax.random.fold_in(keys[12], part), 71), part)
    value_rows = gaussian(part_keys[3], (TOKENS, KV_HEADS * HEAD_DIM), 1.0, 6.0, ((0, 8),))
    seq_lengths = with_ends(jax.random.randint(part_keys[4], (N_EP,), SEQ // 2, SEQ + 1), jax.random.fold_in(part_keys[4], 1), SEQ // 2, SEQ).astype(jnp.int32)
    out_weight = gaussian(keys[5], (HEADS * HEAD_DIM, D), (HEADS * HEAD_DIM) ** -0.5, 0.09375, ((0, 2), (1, 8)))
    norm_gain = jnp.clip(1.0 + 0.15 * jax.random.normal(keys[6], (D,), jnp.float32), 0.25, 1.75)
    expert_ids_keys = jax.random.split(jax.random.fold_in(part_keys[7], 1), TOKENS // SEQ)
    expert_ids_turns = jax.random.permutation(jax.random.fold_in(part_keys[7], 3), TOKENS // SEQ)
    expert_ids = jax.vmap(lambda own, number: routed_block(jax.random.fold_in(part_keys[7], 2), own, number, SEQ, EXPERTS, TOP, CAP, 1))(expert_ids_keys, expert_ids_turns).reshape((TOKENS, TOP))
    gate_probs = jnp.clip(jnp.exp(math.log(0.5) - 2.8134107 * jax.random.uniform(part_keys[8], (TOKENS, TOP), jnp.float32) ** shard_levels(part_keys[8], (TOKENS, TOP), ((0, 8),), -0.2, 0.2)), 0.03, 0.5)
    gate_weight = gaussian(keys[9], (EXPERTS, D, FF), D ** -0.5, 0.09375, ((0, 8), (2, 2)))
    up_weight = gaussian(keys[10], (EXPERTS, D, FF), D ** -0.5, 0.09375, ((0, 8), (2, 2)))
    down_weight = gaussian(keys[11], (EXPERTS, FF, D), FF ** -0.5, 0.15625, ((0, 8), (2, 2)))
    return dict(residual_in=residual_in, queries=queries, key_rows=key_rows, value_rows=value_rows, seq_lengths=seq_lengths, out_weight=out_weight, norm_gain=norm_gain, expert_ids=expert_ids, gate_probs=gate_probs, gate_weight=gate_weight, up_weight=up_weight, down_weight=down_weight)


EPSILON = 1e-06

def attention_all(queries, key_rows, value_rows, seq_lengths):
    group_size = HEADS // KV_HEADS
    query_four = queries.reshape(N_EP, SEQ, HEADS, HEAD_DIM).astype(jnp.float32)
    key_four = key_rows.reshape(N_EP, SEQ, KV_HEADS, HEAD_DIM).astype(jnp.float32)
    value_four = value_rows.reshape(N_EP, SEQ, KV_HEADS, HEAD_DIM).astype(jnp.float32)
    key_heads = jnp.repeat(key_four, group_size, axis=2)
    value_heads = jnp.repeat(value_four, group_size, axis=2)
    scores = jnp.einsum('bqhd,bkhd->bhqk', query_four, key_heads) * HEAD_DIM ** (-0.5)
    positions = jnp.arange(SEQ, dtype=jnp.int32)
    causal = positions[None, :] <= positions[:, None]
    inside = positions[None, None, :] < seq_lengths[:, None, None]
    visible = causal[None, :, :] & inside
    scores = jnp.where(visible[:, None, :, :], scores, jnp.float32(-1e+30))
    row_peak = lax.optimization_barrier(jnp.max(scores, axis=3, keepdims=True))
    exponent = jnp.exp(scores - row_peak)
    weights = (exponent / lax.optimization_barrier(jnp.sum(exponent, axis=3, keepdims=True))).astype(jnp.bfloat16)
    combined = jnp.einsum('bhqk,bkhd->bqhd', weights.astype(jnp.float32), value_heads)
    return combined.astype(jnp.bfloat16).reshape(TOKENS, HEADS * HEAD_DIM)

def expert_apply(operands):
    rows_in, gate_mat, up_mat, down_mat = operands
    gate_val = jnp.dot(rows_in, gate_mat, preferred_element_type=jnp.float32)
    up_val = jnp.dot(rows_in, up_mat, preferred_element_type=jnp.float32)
    hidden_act = (jax.nn.silu(gate_val) * up_val).astype(jnp.bfloat16)
    return jnp.dot(hidden_act, down_mat, preferred_element_type=jnp.float32)

def reference(residual_in, queries, key_rows, value_rows, seq_lengths, out_weight, norm_gain, expert_ids, gate_probs, gate_weight, up_weight, down_weight):
    attended = attention_all(queries, key_rows, value_rows, seq_lengths)
    attn_proj = jnp.dot(attended, out_weight, preferred_element_type=jnp.float32)
    residual = (residual_in.astype(jnp.float32) + attn_proj).astype(jnp.bfloat16)
    residual_wide = residual.astype(jnp.float32)
    mean_square = lax.optimization_barrier(jnp.sum(residual_wide * residual_wide, axis=1)) / D
    normed = (residual_wide * lax.rsqrt(mean_square + EPSILON)[:, None] * norm_gain).astype(jnp.bfloat16)
    block_ids = expert_ids.reshape(N_EP, SEQ * TOP).astype(jnp.int32)
    one_hot = (block_ids[:, :, None] == jnp.arange(EXPERTS, dtype=jnp.int32)[None, None, :]).astype(jnp.int32)
    earlier = jnp.cumsum(one_hot, axis=1) - one_hot
    slot_rank = lax.optimization_barrier(jnp.sum(earlier * one_hot, axis=2))
    block_index = jnp.arange(N_EP, dtype=jnp.int32)[:, None]
    target = ((block_ids * N_EP + block_index) * CAP + slot_rank).reshape(-1).astype(jnp.int32)
    pair_token = (block_index * SEQ + jnp.arange(SEQ * TOP, dtype=jnp.int32)[None, :] // TOP).reshape(-1).astype(jnp.int32)
    token_of = jnp.zeros((EXPERTS * N_EP * CAP,), jnp.int32).at[target].set(pair_token)
    filled = jnp.zeros((EXPERTS * N_EP * CAP,), jnp.bool_).at[target].set(True)
    taken = jnp.where(filled[:, None], jnp.take(normed, token_of, axis=0), jnp.zeros((), jnp.bfloat16))
    taken = taken.reshape(EXPERTS, N_EP * CAP, D)
    produced = lax.map(expert_apply, (taken, gate_weight, up_weight, down_weight))
    picked = jnp.take(produced.reshape(EXPERTS * N_EP * CAP, D), target, axis=0).reshape(TOKENS, TOP, D)
    mixture = jnp.einsum('tk,tkd->td', gate_probs.astype(jnp.float32), picked, precision=lax.Precision.HIGHEST)
    return (residual_wide + mixture).astype(jnp.bfloat16)
```

```python
import jax
import jax.numpy as jnp
from jax import lax
from jax.sharding import PartitionSpec as P


D = 4096
HEADS = 32
KV_HEADS = 2
HEAD_DIM = 128


EPSILON = 1e-06


def attend(queries, key_rows, value_rows, seq_lengths):
    seq_rows = queries.shape[0]
    heads_here = queries.shape[1] // HEAD_DIM
    group_size = HEADS // KV_HEADS
    kv_column = lax.axis_index("tp") * heads_here // group_size * HEAD_DIM
    key_head = lax.dynamic_slice_in_dim(key_rows, kv_column, HEAD_DIM, 1)
    value_head = lax.dynamic_slice_in_dim(value_rows, kv_column, HEAD_DIM, 1)
    query_three = queries.reshape(seq_rows, heads_here, HEAD_DIM)
    scores = jnp.einsum(
        "qhd,kd->hqk", query_three, key_head, preferred_element_type=jnp.float32
    ) * HEAD_DIM ** (-0.5)
    positions = jnp.arange(seq_rows, dtype=jnp.int32)
    visible = (positions[None, :] <= positions[:, None]) & (positions[None, :] < seq_lengths[0])
    scores = jnp.where(visible[None, :, :], scores, jnp.float32(-1e30))
    row_peak = jnp.max(scores, axis=2, keepdims=True)
    exponent = jnp.exp(scores - row_peak)
    weights = (exponent / jnp.sum(exponent, axis=2, keepdims=True)).astype(jnp.bfloat16)
    combined = jnp.einsum("hqk,kd->qhd", weights, value_head, preferred_element_type=jnp.float32)
    return combined.astype(jnp.bfloat16).reshape(seq_rows, heads_here * HEAD_DIM)


def ring_of(count):
    return list(range(0, count, 2)) + list(range(1, count, 2))[::-1]


def ring_send(value, shift):
    order = ring_of(lax.axis_size("ep"))
    count = len(order)
    pairs = [(order[i], order[(i + shift) % count]) for i in range(count)]
    return lax.ppermute(value, "ep", pairs)


def core_gather(value):
    count = lax.axis_size("tp")
    if count != 2:
        return lax.all_gather(value, "tp", axis=value.ndim - 1, tiled=True)
    other = lax.ppermute(value, "tp", [(0, 1), (1, 0)])
    first = lax.axis_index("tp") == 0
    return jnp.concatenate(
        [jnp.where(first, value, other), jnp.where(first, other, value)], axis=value.ndim - 1
    )


def core_scatter(value):
    count = lax.axis_size("tp")
    rounded = value.astype(jnp.bfloat16)
    if count != 2:
        return lax.psum_scatter(rounded, "tp", scatter_dimension=1, tiled=True).astype(jnp.float32)
    half = value.shape[1] // 2
    first = lax.axis_index("tp") == 0
    left, right = value[:, :half], value[:, half:]
    arrived = lax.ppermute(
        jnp.where(first, rounded[:, half:], rounded[:, :half]), "tp", [(0, 1), (1, 0)]
    )
    return jnp.where(first, left, right) + arrived.astype(jnp.float32)


def ring_gather(block):
    half = lax.axis_size("ep") // 2
    rows = block.shape[0] // 2
    ahead, behind = [block], [block]
    for _ in range(1, half):
        ahead.append(ring_send(ahead[-1], 1))
        behind.append(ring_send(behind[-1], -1))
    far = jnp.concatenate(
        [ring_send(ahead[-1][:rows], 1), ring_send(behind[-1][rows:], -1)], axis=0
    )
    return ahead, behind, far


def project_out(attended, out_weight):
    ep_count = lax.axis_size("ep")
    tp_count = lax.axis_size("tp")
    order = ring_of(ep_count)
    half = ep_count // 2
    seq_rows = attended.shape[0]
    ahead, behind, far = ring_gather(attended)
    share = out_weight.shape[1] // tp_count
    place = ring_place()

    def part(rows):
        total = jnp.dot(rows, out_weight, preferred_element_type=jnp.float32)
        return core_scatter(total).astype(jnp.bfloat16)

    pieces = [None] * ep_count
    pieces[0] = part(attended)
    for j in range(1, half):
        both = part(jnp.concatenate([ahead[j], behind[j]], axis=0))
        pieces[(-j) % ep_count] = both[:seq_rows]
        pieces[j] = both[seq_rows:]
    pieces[half] = part(far)
    stacked = jnp.stack(pieces)
    group = ep_count // tp_count
    slot = (lax.axis_index("ep") % group) * tp_count + lax.axis_index("tp")
    table = jnp.asarray([order.index(e) for e in range(ep_count)], jnp.int32)
    arrivals = []
    for k in range(ep_count):
        goal = (slot + k) % ep_count
        distance = (table[goal] - place) % ep_count
        message = lax.dynamic_index_in_dim(stacked, distance, 0, keepdims=False)
        pairs = []
        for e in range(ep_count):
            for c in range(tp_count):
                to = ((e % group) * tp_count + c + k) % ep_count
                pairs.append((e * tp_count + c, to * tp_count + e // group))
        arrivals.append(lax.ppermute(message, ("ep", "tp"), pairs))
    mine = lax.axis_index("ep")
    gathered = jnp.stack([arrivals[k] for k in range(ep_count)][::-1], axis=1)
    doubled = jnp.concatenate([gathered, gathered], axis=1)
    start = (ep_count - 1 - mine) % ep_count
    sorted_slots = lax.dynamic_slice_in_dim(doubled, start, ep_count, 1)
    return sorted_slots.reshape(seq_rows, ep_count * share).astype(jnp.float32)


def ring_place():
    order = ring_of(lax.axis_size("ep"))
    table = jnp.asarray([order.index(e) for e in range(len(order))], jnp.int32)
    return table[lax.axis_index("ep")]


def shards(
    residual_in,
    queries,
    key_rows,
    value_rows,
    seq_lengths,
    out_weight,
    norm_gain,
    expert_ids,
    gate_probs,
    gate_weight,
    up_weight,
    down_weight,
):
    seq_rows = residual_in.shape[0]
    local_experts = gate_weight.shape[0]
    ep_count = lax.axis_size("ep")
    expert_count = local_experts * ep_count
    half = ep_count // 2
    chosen = expert_ids[:, :, None] == jnp.arange(expert_count, dtype=jnp.int32)[None, None, :]
    spread = jnp.sum(jnp.where(chosen, gate_probs[:, :, None], 0.0), axis=1)

    def own_columns(table):
        return lax.dynamic_slice_in_dim(
            table, lax.axis_index("ep") * local_experts, local_experts, 1
        )

    weights_at = [own_columns(ring_send(spread, d) if d else spread) for d in range(ep_count)]

    attended = attend(queries, key_rows, value_rows, seq_lengths)
    head_total = project_out(attended, out_weight)
    residual = (residual_in.astype(jnp.float32) + head_total).astype(jnp.bfloat16)
    residual_wide = residual.astype(jnp.float32)
    square_sum = jnp.sum(residual_wide * residual_wide, axis=1, keepdims=True)
    square_sum = jnp.sum(core_gather(square_sum), axis=1)
    mean_square = square_sum / D
    normed = (residual_wide * lax.rsqrt(mean_square + EPSILON)[:, None] * norm_gain).astype(
        jnp.bfloat16
    )

    def hidden_of(rows, scale):
        whole = core_gather(rows)
        outs = []
        for e in range(local_experts):
            gate_val = jnp.dot(whole, gate_weight[e], preferred_element_type=jnp.float32)
            up_val = jnp.dot(whole, up_weight[e], preferred_element_type=jnp.float32)
            active = jax.nn.silu(gate_val) * up_val * scale[:, e : e + 1]
            outs.append(active.astype(jnp.bfloat16))
        joined = core_gather(jnp.stack(outs))
        return [joined[e] for e in range(local_experts)]

    def produced(hiddens):
        total = None
        for e in range(local_experts):
            term = jnp.dot(hiddens[e], down_weight[e], preferred_element_type=jnp.float32)
            total = term if total is None else total + term
        return total

    ahead, behind, far = ring_gather(normed)
    own = hidden_of(normed, weights_at[0])
    pairs = [None]
    for j in range(1, half):
        pairs.append(
            hidden_of(
                jnp.concatenate([ahead[j], behind[j]], axis=0),
                jnp.concatenate([weights_at[j], weights_at[ep_count - j]], axis=0),
            )
        )
    last = produced(hidden_of(far, weights_at[half]))
    back = ring_send(last[: seq_rows // 2].astype(jnp.bfloat16), -1)
    onward = ring_send(last[seq_rows // 2 :].astype(jnp.bfloat16), 1)
    for j in range(half - 1, 0, -1):
        both = produced(pairs[j])
        to_back, to_on = both[:seq_rows], both[seq_rows:]
        if j == half - 1:
            rows = seq_rows // 2
            to_back = to_back + jnp.pad(back.astype(jnp.float32), ((0, rows), (0, 0)))
            to_on = to_on + jnp.pad(onward.astype(jnp.float32), ((rows, 0), (0, 0)))
        else:
            to_back = to_back + back.astype(jnp.float32)
            to_on = to_on + onward.astype(jnp.float32)
        back = ring_send(to_back.astype(jnp.bfloat16), -1)
        onward = ring_send(to_on.astype(jnp.bfloat16), 1)
    mixture = produced(own) + back.astype(jnp.float32) + onward.astype(jnp.float32)
    return (residual_wide + mixture).astype(jnp.bfloat16)


def solution(mesh):
    return jax.shard_map(
        shards,
        mesh=mesh,
        in_specs=(
            P(("rep", "ep"), "tp"),
            P(("rep", "ep"), "tp"),
            P(("rep", "ep"), None),
            P(("rep", "ep"), None),
            P(("rep", "ep")),
            P("tp", "ep"),
            P("tp"),
            P(("rep", "ep"), None),
            P(("rep", "ep"), None),
            P("ep", None, "tp"),
            P("ep", None, "tp"),
            P("ep", None, "tp"),
        ),
        out_specs=P(("rep", "ep"), "tp"),
        check_vma=False,
    )
```

```python
import functools

import jax
import jax.numpy as jnp
from jax import lax
from jax.experimental import pallas as pl
from jax.experimental.pallas import tpu as pltpu
from jax.sharding import PartitionSpec as P


D = 4096
HEADS = 32
KV_HEADS = 2
HEAD_DIM = 128


EPSILON = 1e-06


def attend(queries, key_rows, value_rows, seq_lengths):
    seq_rows = queries.shape[0]
    heads_here = queries.shape[1] // HEAD_DIM
    group_size = HEADS // KV_HEADS
    kv_column = lax.axis_index("tp") * heads_here // group_size * HEAD_DIM
    key_head = lax.dynamic_slice_in_dim(key_rows, kv_column, HEAD_DIM, 1)
    value_head = lax.dynamic_slice_in_dim(value_rows, kv_column, HEAD_DIM, 1)
    query_three = queries.reshape(seq_rows, heads_here, HEAD_DIM)
    scores = jnp.einsum(
        "qhd,kd->hqk", query_three, key_head, preferred_element_type=jnp.float32
    ) * HEAD_DIM ** (-0.5)
    positions = jnp.arange(seq_rows, dtype=jnp.int32)
    visible = (positions[None, :] <= positions[:, None]) & (positions[None, :] < seq_lengths[0])
    scores = jnp.where(visible[None, :, :], scores, jnp.float32(-1e30))
    row_peak = jnp.max(scores, axis=2, keepdims=True)
    exponent = jnp.exp(scores - row_peak)
    weights = (exponent / jnp.sum(exponent, axis=2, keepdims=True)).astype(jnp.bfloat16)
    combined = jnp.einsum("hqk,kd->qhd", weights, value_head, preferred_element_type=jnp.float32)
    return combined.astype(jnp.bfloat16).reshape(seq_rows, heads_here * HEAD_DIM)


def ring_of(count):
    return list(range(0, count, 2)) + list(range(1, count, 2))[::-1]


def ring_send(value, shift):
    order = ring_of(lax.axis_size("ep"))
    count = len(order)
    pairs = [(order[i], order[(i + shift) % count]) for i in range(count)]
    return lax.ppermute(value, "ep", pairs)


def core_gather(value):
    count = lax.axis_size("tp")
    if count != 2:
        return lax.all_gather(value, "tp", axis=value.ndim - 1, tiled=True)
    other = lax.ppermute(value, "tp", [(0, 1), (1, 0)])
    first = lax.axis_index("tp") == 0
    return jnp.concatenate(
        [jnp.where(first, value, other), jnp.where(first, other, value)], axis=value.ndim - 1
    )


def core_scatter(value):
    count = lax.axis_size("tp")
    rounded = value.astype(jnp.bfloat16)
    if count != 2:
        return lax.psum_scatter(rounded, "tp", scatter_dimension=1, tiled=True).astype(jnp.float32)
    half = value.shape[1] // 2
    first = lax.axis_index("tp") == 0
    left, right = value[:, :half], value[:, half:]
    arrived = lax.ppermute(
        jnp.where(first, rounded[:, half:], rounded[:, :half]), "tp", [(0, 1), (1, 0)]
    )
    return jnp.where(first, left, right) + arrived.astype(jnp.float32)


MESH = pl.DeviceIdType.MESH


def place_of(index, count):
    return index // 2 + (index % 2) * (count - 1 - 2 * (index // 2))


def ring_at(place, count):
    return 2 * place + (place // (count // 2)) * (2 * count - 1 - 4 * place)


def gather_kernel(count, arrays, *refs):
    ins, outs = refs[:arrays], refs[arrays : 2 * arrays]
    send_sem, recv_sem, local_sem = refs[2 * arrays :]
    half = count // 2
    place = place_of(lax.axis_index("ep"), count)
    right = ring_at((place + 1) % count, count)
    left = ring_at((place + count - 1) % count, count)
    barrier = pltpu.get_barrier_semaphore()
    for neighbour in (left, right):
        pl.semaphore_signal(barrier, inc=1, device_id={"ep": neighbour}, device_id_type=MESH)
    pl.semaphore_wait(barrier, 2)

    def send(n, way, step, source, target):
        copy = pltpu.make_async_remote_copy(
            src_ref=source,
            dst_ref=target,
            send_sem=send_sem.at[n, way, step],
            recv_sem=recv_sem.at[n, way, step],
            device_id={"ep": left if way else right},
            device_id_type=MESH,
        )
        copy.start()
        return copy

    copies, latest, own = [], {}, []
    for step in range(half):
        for n in range(arrays):
            for way in (0, 1):
                at = (count - step) % count if way else step
                to = (at - 1) % count if way else at + 1
                source = outs[n].at[at] if step else ins[n]
                target = outs[n].at[to]
                if step:
                    latest[n, way].wait_recv()
                if step == half - 1:
                    if n:
                        if way:
                            continue
                    else:
                        rows = ins[n].shape[0] // 2
                        span = pl.ds(rows * way, rows)
                        source, target = source.at[span], target.at[span]
                latest[n, way] = send(n, way, step, source, target)
                copies.append((n, way, step, latest[n, way]))
        if step == 0:
            for n in range(arrays):
                own.append(pltpu.make_async_copy(ins[n], outs[n].at[0], local_sem.at[n]))
                own[-1].start()
    for copy in own:
        copy.wait()
    for n, way, step, copy in copies:
        if step == half - 1:
            copy.wait_recv()
    for n, way, step, copy in copies:
        copy.wait_send()


def ring_gather(arrays, number):
    count = lax.axis_size("ep")
    kept = pl.BlockSpec(memory_space=pltpu.VMEM)
    sems = pltpu.SemaphoreType.DMA((len(arrays), 2, count // 2))
    return pl.pallas_call(
        functools.partial(gather_kernel, count, len(arrays)),
        out_shape=[jax.ShapeDtypeStruct((count,) + a.shape, a.dtype) for a in arrays],
        in_specs=[kept] * len(arrays),
        out_specs=[kept] * len(arrays),
        scratch_shapes=[sems, sems, pltpu.SemaphoreType.DMA((len(arrays),))],
        compiler_params=pltpu.CompilerParams(
            collective_id=number, has_side_effects=True, vmem_limit_bytes=48 * 1024 * 1024
        ),
    )(*arrays)


def return_kernel(ep_count, tp_count, x_ref, out_ref, send_sem, recv_sem, local_sem):
    group = ep_count // tp_count
    e, c = lax.axis_index("ep"), lax.axis_index("tp")
    owner = e // group
    slot = (e % group) * tp_count + c
    place = place_of(e, ep_count)
    barrier = pltpu.get_barrier_semaphore()
    mine = []
    for k in range(ep_count):
        mine.append(((slot + k) % ep_count == e) & (owner == c))
        giver = (e + ep_count - k) % ep_count

        @pl.when(jnp.logical_not(mine[k]))
        def _():
            pl.semaphore_signal(
                barrier,
                inc=1,
                device_id={"ep": c * group + giver // tp_count, "tp": giver % tp_count},
                device_id_type=MESH,
            )

    @pl.when(owner == c)
    def _():
        pl.semaphore_wait(barrier, ep_count - 1)

    @pl.when(owner != c)
    def _():
        pl.semaphore_wait(barrier, ep_count)

    def copy_of(k):
        goal = (slot + k) % ep_count
        distance = (place + ep_count - place_of(goal, ep_count)) % ep_count
        return pltpu.make_async_remote_copy(
            src_ref=x_ref.at[distance],
            dst_ref=out_ref.at[slot],
            send_sem=send_sem.at[k],
            recv_sem=recv_sem.at[k],
            device_id={"ep": goal, "tp": owner},
            device_id_type=MESH,
        )

    for k in range(ep_count):

        @pl.when(jnp.logical_not(mine[k]))
        def _():
            copy_of(k).start()

        @pl.when(mine[k])
        def _():
            own = pltpu.make_async_copy(x_ref.at[0], out_ref.at[slot], local_sem)
            own.start()
            own.wait()

    for k in range(ep_count):

        @pl.when(jnp.logical_not(mine[k]))
        def _():
            copy_of(k).wait()


def project_out(gathered, out_weight):
    ep_count = lax.axis_size("ep")
    tp_count = lax.axis_size("tp")
    seq_rows = gathered.shape[1]
    total = jnp.dot(
        gathered.reshape(ep_count * seq_rows, gathered.shape[2]),
        out_weight,
        preferred_element_type=jnp.float32,
    )
    share = out_weight.shape[1] // tp_count
    pieces = core_scatter(total).astype(jnp.bfloat16).reshape(ep_count, seq_rows, share)
    kept = pl.BlockSpec(memory_space=pltpu.VMEM)
    arrived = pl.pallas_call(
        functools.partial(return_kernel, ep_count, tp_count),
        out_shape=jax.ShapeDtypeStruct(pieces.shape, pieces.dtype),
        in_specs=[kept],
        out_specs=kept,
        scratch_shapes=[
            pltpu.SemaphoreType.DMA((ep_count,)),
            pltpu.SemaphoreType.DMA((ep_count,)),
            pltpu.SemaphoreType.DMA,
        ],
        compiler_params=pltpu.CompilerParams(collective_id=1, has_side_effects=True),
    )(pieces)
    return arrived.transpose(1, 0, 2).reshape(seq_rows, ep_count * share).astype(jnp.float32)


def shards(
    residual_in,
    queries,
    key_rows,
    value_rows,
    seq_lengths,
    out_weight,
    norm_gain,
    expert_ids,
    gate_probs,
    gate_weight,
    up_weight,
    down_weight,
):
    seq_rows = residual_in.shape[0]
    local_experts = gate_weight.shape[0]
    ep_count = lax.axis_size("ep")
    expert_count = local_experts * ep_count
    half = ep_count // 2
    chosen = expert_ids[:, :, None] == jnp.arange(expert_count, dtype=jnp.int32)[None, None, :]
    spread = jnp.sum(jnp.where(chosen, gate_probs[:, :, None], 0.0), axis=1)

    attended = attend(queries, key_rows, value_rows, seq_lengths)
    gathered, spreads = ring_gather([attended, spread.T], 0)
    head_total = project_out(gathered, out_weight)
    scales = lax.dynamic_slice_in_dim(
        spreads, lax.axis_index("ep") * local_experts, local_experts, 1
    ).transpose(0, 2, 1)
    residual = (residual_in.astype(jnp.float32) + head_total).astype(jnp.bfloat16)
    residual_wide = residual.astype(jnp.float32)
    square_sum = jnp.sum(residual_wide * residual_wide, axis=1, keepdims=True)
    square_sum = jnp.sum(core_gather(square_sum), axis=1)
    mean_square = square_sum / D
    normed = (residual_wide * lax.rsqrt(mean_square + EPSILON)[:, None] * norm_gain).astype(
        jnp.bfloat16
    )

    def hidden_of(rows, scale):
        whole = core_gather(rows)
        outs = []
        for e in range(local_experts):
            gate_val = jnp.dot(whole, gate_weight[e], preferred_element_type=jnp.float32)
            up_val = jnp.dot(whole, up_weight[e], preferred_element_type=jnp.float32)
            active = jax.nn.silu(gate_val) * up_val * scale[:, e : e + 1]
            outs.append(active.astype(jnp.bfloat16))
        joined = core_gather(jnp.stack(outs))
        return [joined[e] for e in range(local_experts)]

    def produced(hiddens):
        total = None
        for e in range(local_experts):
            term = jnp.dot(hiddens[e], down_weight[e], preferred_element_type=jnp.float32)
            total = term if total is None else total + term
        return total

    (arrived,) = ring_gather([normed], 2)
    width = normed.shape[1]

    def chunk(first):
        rows = arrived[first : first + half].reshape(half * seq_rows, width)
        scale = scales[first : first + half].reshape(half * seq_rows, local_experts)
        return hidden_of(rows, scale)

    later, early = chunk(half), chunk(0)

    def at(distance):
        source = later if distance >= half else early
        start = distance % half * seq_rows
        return [h[start : start + seq_rows] for h in source]

    pairs = [
        [jnp.concatenate([u, v], axis=0) for u, v in zip(at(j), at((-j) % ep_count))]
        for j in range(half)
    ]
    own = at(0)
    last = produced(at(half))
    back = ring_send(last[: seq_rows // 2].astype(jnp.bfloat16), -1)
    onward = ring_send(last[seq_rows // 2 :].astype(jnp.bfloat16), 1)
    for j in range(half - 1, 0, -1):
        both = produced(pairs[j])
        to_back, to_on = both[:seq_rows], both[seq_rows:]
        if j == half - 1:
            rows = seq_rows // 2
            to_back = to_back + jnp.pad(back.astype(jnp.float32), ((0, rows), (0, 0)))
            to_on = to_on + jnp.pad(onward.astype(jnp.float32), ((rows, 0), (0, 0)))
        else:
            to_back = to_back + back.astype(jnp.float32)
            to_on = to_on + onward.astype(jnp.float32)
        back = ring_send(to_back.astype(jnp.bfloat16), -1)
        onward = ring_send(to_on.astype(jnp.bfloat16), 1)
    mixture = produced(own) + back.astype(jnp.float32) + onward.astype(jnp.float32)
    return (residual_wide + mixture).astype(jnp.bfloat16)


def solution(mesh):
    return jax.shard_map(
        shards,
        mesh=mesh,
        in_specs=(
            P(("rep", "ep"), "tp"),
            P(("rep", "ep"), "tp"),
            P(("rep", "ep"), None),
            P(("rep", "ep"), None),
            P(("rep", "ep")),
            P("tp", "ep"),
            P("tp"),
            P(("rep", "ep"), None),
            P(("rep", "ep"), None),
            P("ep", None, "tp"),
            P("ep", None, "tp"),
            P("ep", None, "tp"),
        ),
        out_specs=P(("rep", "ep"), "tp"),
        check_vma=False,
    )
```
